32 devices in a mesh: rowa: 2 (over x), rowb: 4 (over z), col: 4 (over y, core).
Axes of the slice: x: 2, y: 2, z: 4, core: 2. Of those that a mesh axis runs over, the one named last changes fastest.
Arguments:
- table: float32 [65536, 512], P(('rowa', 'rowb'), 'col'), may hold values from -12 to 12
- start: float32 [16, 512], P(None, 'col'), may hold values from -6 to 6
Outputs:
- right_vectors: float32 [16, 512], P(None, 'col')
- left_images: float32 [16, 65536], P(None, ('rowa', 'rowb'))
- strengths: float32 [16], replicated
The draws below stay inside these ranges and needn't reach their ends.
All inputs are finite; a program needn't handle non-finite values.
Results may differ from the reference program's by a relative error of at most 0.00014.
Values sent between devices are 32-bit elements.
A program may use at most 64 MiB of HBM per device.

```python
import jax
import jax.numpy as jnp
from jax import lax

COLS = 512
BLOCK = 16
STEPS = 8
ROW_DEV = 8192
ROWS = 65536


def draw_table(key, part):
    key_noise, key_scale, key_lead, key_amount = jax.random.split(jax.random.fold_in(key, 17), 4)
    blocks = ROWS // ROW_DEV
    col_scale = jnp.exp(jax.random.uniform(key_scale, (COLS,), jnp.float32, -0.6931472, 0.6931472))
    noise = jax.random.normal(key_noise, (blocks, ROW_DEV, COLS), jnp.float32)
    weight = 0.5
    lead = jax.random.normal(key_lead, (blocks, 1, COLS), jnp.float32) * weight
    amount = jax.random.normal(key_amount, (blocks, ROW_DEV, 1), jnp.float32)
    table = noise * col_scale + amount * lead
    return jnp.clip(table, -12.0, 12.0).reshape(ROWS, COLS)


def steps_of(own_key, extent, shards, smallest, largest):
    level = 1.0
    for position, shards_of in shards:
        draws = jax.random.uniform(jax.random.fold_in(jax.random.fold_in(own_key, 6), position), (shards_of,), jnp.float32, smallest / len(shards), largest / len(shards))
        level = level * jnp.repeat(jnp.exp(draws), extent[position] // shards_of).reshape((-1,) + (1,) * (len(extent) - 1 - position))
    return level


def normal_values(own_key, shape, width, reach, pieces=(), held_as=jnp.bfloat16):
    values = width * jax.random.normal(own_key, shape, jnp.float32)
    if pieces:
        values = values * steps_of(own_key, shape, pieces, -0.22, 0.18)
    return jnp.clip(values, -reach, reach).astype(held_as)


def setup_inputs(seed: int = 0) -> dict:
    streams_of = jax.random.split(jax.random.key(seed), 3)
    table = draw_table(jax.random.fold_in(streams_of[2], 71), 0)
    start = normal_values(streams_of[1], (BLOCK, COLS), 1.0, 6.0, ((1, 4),), jnp.float32)
    return dict(table=table, start=start)


high = lax.Precision.HIGHEST

def reference(table, start):
    vectors = start
    images = None
    lower = None
    for step in range(STEPS):
        images = lax.dot_general(vectors.astype(jnp.float32), table.astype(jnp.float32), (((1,), (1,)), ((), ())), precision=high, preferred_element_type=jnp.float32)
        products = jnp.dot(images.astype(jnp.float32), table.astype(jnp.float32), precision=high, preferred_element_type=jnp.float32)
        gram = lax.dot_general(products.astype(jnp.float32), products.astype(jnp.float32), (((1,), (1,)), ((), ())), precision=high, preferred_element_type=jnp.float32)
        lower = jnp.linalg.cholesky(gram)
        vectors = jax.scipy.linalg.solve_triangular(lower, products, lower=True)
    strengths = jnp.diagonal(lower) / ROWS
    return (vectors, images, strengths)
```

```python
import functools

import jax
import jax.numpy as jnp
from jax import lax
from jax.experimental import pallas as pl
from jax.experimental.pallas import tpu as pltpu
from jax.sharding import PartitionSpec as P

STEPS = 8
CHUNKS = 8
LEFT_CHUNKS = 4
CORES = 2
MESH = pl.DeviceIdType.MESH
high = lax.Precision.HIGHEST


def dot(a, b, dims):
    return lax.dot_general(a, b, (dims, ((), ())), precision=high, preferred_element_type=jnp.float32)


def orthonormal(products):
    block, cols = products.shape
    tiles = cols // 128
    gram = dot(products, products, ((1,), (1,)))
    column = [jnp.broadcast_to(gram[:, k : k + 1], (block, 128)) for k in range(block)]
    part = [products[:, t * 128 : (t + 1) * 128] for t in range(tiles)]
    row = lax.broadcasted_iota(jnp.int32, (block, 128), 0)
    lane = lax.broadcasted_iota(jnp.int32, (1, 128), 1)
    diagonal = jnp.zeros((1, 128), jnp.float32)
    for j in range(block):
        pivot = column[j][j : j + 1, :]
        inverse = lax.rsqrt(pivot)
        inverse = inverse * (1.5 - 0.5 * (pivot * inverse) * inverse)
        diagonal = jnp.where(lane == j, pivot * inverse, diagonal)
        below = jnp.where(row > j, column[j] * inverse, 0.0)
        for t in range(tiles):
            solved = part[t][j : j + 1, :] * inverse
            part[t] = jnp.where(row == j, solved, part[t] - below * solved)
        for k in range(j + 1, block):
            column[k] = column[k] - below * below[k : k + 1, :]
    return jnp.concatenate(part, axis=1), diagonal


def kernel(na, nb, nc, n_copies, table, start, right_ref, left_ref, strength_ref, *scratch):
    (blocks, extra, vecs, acc_d, acc_c, diag, cross, cover,
     d_core, d_a, d_b, c_core, c_hi, c_a, c_b, send, recv, local) = scratch
    nh = nc // CORES
    rows_dev, width = table.shape
    quarter = rows_dev // nc
    chunk = quarter // CHUNKS
    half = CORES * width
    a, b, col = lax.axis_index("rowa"), lax.axis_index("rowb"), lax.axis_index("col")
    core, hi = lax.rem(col, CORES), lax.div(col, CORES)
    at_a = lambda i: {"rowa": i}
    at_b = lambda i: {"rowb": i}
    at_col = lambda i: {"col": i}
    at_core = lambda i: {"col": hi * CORES + i}
    at_hi = lambda i: {"col": i * CORES + core}
    used = [0]

    barrier = pltpu.get_barrier_semaphore()
    others = ([at_a(lax.rem(a + d, na)) for d in range(1, na)] + [at_b(lax.rem(b + d, nb)) for d in range(1, nb)]
              + [at_col(lax.rem(col + d, nc)) for d in range(1, nc)])
    for other in others:
        pl.semaphore_signal(barrier, inc=1, device_id=other, device_id_type=MESH)
    pl.semaphore_wait(barrier, len(others))

    def remote(src, dst, where):
        i = used[0]
        used[0] += 1
        copy = pltpu.make_async_remote_copy(src_ref=src, dst_ref=dst, send_sem=send.at[i], recv_sem=recv.at[i],
                                            device_id=where, device_id_type=MESH)
        copy.start()
        return copy

    def aligned(x, n):
        return pl.multiple_of(x, n)

    copies = [pltpu.make_async_copy(table.at[pl.ds(aligned(col * quarter, 8), quarter)], blocks.at[col], local.at[0])]
    for h in range(1, nh):
        q = lax.rem(hi + h, nh) * CORES + core
        copies.append(pltpu.make_async_copy(table.at[pl.ds(aligned(q * quarter, 8), quarter)], extra.at[h - 1, core], local.at[h]))
    for c in copies:
        c.start()
    near = []
    peer = 1 - core
    q = hi * CORES + peer
    near.append(remote(table.at[pl.ds(aligned(q * quarter, 8), quarter)], blocks.at[col], at_core(peer)))
    for h in range(1, nh):
        q = lax.rem(hi + h, nh) * CORES + peer
        near.append(remote(table.at[pl.ds(aligned(q * quarter, 8), quarter)], extra.at[h - 1, core], at_core(peer)))
    vecs[col] = start[...]
    for d in range(1, nc):
        near.append(remote(start, vecs.at[col], at_col(lax.rem(col + d, nc))))
    far = []
    for k in range(CHUNKS):
        far.append([])
        for h in range(1, nh):
            for c in range(CORES):
                q = lax.rem(hi + h, nh) * CORES + lax.rem(core + c, CORES)
                far[k].append(remote(table.at[pl.ds(aligned(q * quarter + k * chunk, 8), chunk)],
                                     blocks.at[col, pl.ds(k * chunk, chunk)], at_col(q)))

    def allreduce(acc, out, stages, slots, over_b, gather):
        off, length = 0, half
        trail = []
        for (n, me, at), slot in zip(stages, slots):
            piece = length // n
            moved = []
            for d in range(1, n):
                to = lax.rem(me + d, n)
                moved.append(remote(acc.at[pl.ds(aligned(off + to * piece, 8), piece)], slot.at[d - 1], at(to)))
            yield
            for m in moved:
                m.wait()
            trail.append((off, length))
            off, length = off + me * piece, piece
            mine = pl.ds(aligned(off, 8), length)
            total = acc[mine]
            for d in range(1, n):
                total = total + slot[d - 1]
            acc[mine] = total
        mine = pl.ds(aligned(off, 8), length)
        over_b[b] = acc[mine]
        moved = [remote(over_b.at[b], over_b.at[b], at_b(lax.rem(b + d, nb))) for d in range(1, nb)]
        yield
        for m in moved:
            m.wait()
        total = over_b[0]
        for i in range(1, nb):
            total = total + over_b[i]
        out[mine] = total
        for (n, me, at), (above, longer) in list(zip(stages, trail))[::-1][:gather]:
            mine = pl.ds(aligned(off, 8), length)
            moved = [remote(out.at[mine], out.at[mine], at(lax.rem(me + d, n))) for d in range(1, n)]
            yield
            for m in moved:
                m.wait()
            off, length = above, longer

    def diagonal_parts():
        acc_d[...] = jnp.zeros_like(acc_d)
        for c in copies:
            c.wait()
        for n in near:
            n.wait()

        @pl.loop(0, CHUNKS)
        def _(k):
            rows = pl.ds(aligned(k * chunk, 8), chunk)
            own = jnp.concatenate([blocks[hi * CORES + i, rows] for i in range(CORES)], axis=1)
            total = acc_d[...] + dot(own, own, ((0,), (0,)))
            for h in range(1, nh):
                own = jnp.concatenate([extra[h - 1, i, rows] for i in range(CORES)], axis=1)
                total = total + dot(own, own, ((0,), (0,)))
            acc_d[...] = total

        mine = diag.at[hi]
        yield from allreduce(acc_d, mine, [(CORES, core, at_core), (na, a, at_a)], [d_core, d_a], d_b, 1)
        rows = pl.ds(aligned(core * (half // CORES), 8), half // CORES)
        moved = [remote(mine.at[rows], mine.at[rows], at_hi(lax.rem(hi + h, nh))) for h in range(1, nh)]
        yield
        for m in moved:
            m.wait()
        moved = [remote(diag.at[:, rows], diag.at[:, rows], at_core(peer))]
        yield
        for m in moved:
            m.wait()

    def cross_chunk(k):
        for m in far[k]:
            m.wait()
        rows = pl.ds(k * chunk, chunk)
        left = jnp.concatenate([blocks[i, rows] for i in range(CORES)], axis=1)
        rest = jnp.concatenate([blocks[i, rows] for i in range(CORES, nc)], axis=1)
        new = dot(left, rest, ((0,), (0,)))
        acc_c[...] = new if k == 0 else acc_c[...] + new

    beside = diagonal_parts()
    next(beside)
    for k in range(CHUNKS):
        cross_chunk(k)
        if k < CHUNKS - 1 and k < 4:
            next(beside)
    stages = [(CORES, core, at_core), (nh, hi, at_hi), (na, a, at_a)]
    for i, _ in enumerate(allreduce(acc_c, cross, stages, [c_core, c_hi, c_a], c_b, 3)):
        if i == 4:
            next(beside)
    for _ in beside:
        pass
    for h in range(nh):
        cover[h * half : (h + 1) * half, h * half : (h + 1) * half] = diag[h]
    cover[:half, half:] = cross[...]
    cover[half:, :half] = cross[...].T

    vectors = jnp.concatenate([vecs[i] for i in range(nc)], axis=1)

    def step(_, vectors):
        return orthonormal(dot(vectors, cover[...], ((1,), (0,))))[0]

    previous = lax.fori_loop(0, STEPS - 1, step, vectors)
    moved, sent = [], []
    rows = quarter // LEFT_CHUNKS
    for k in range(LEFT_CHUNKS):
        piece = jnp.concatenate([blocks[i, pl.ds(k * rows, rows)] for i in range(nc)], axis=1)
        place = pl.ds(aligned(col * quarter + k * rows, 128), rows)
        left_ref[:, place] = dot(previous, piece, ((1,), (1,)))
        moved.append([remote(left_ref.at[:, place], left_ref.at[:, place], at_hi(lax.rem(hi + h, nh))) for h in range(1, nh)])
        sent.append(remote(left_ref.at[:, place], left_ref.at[:, place], at_core(peer)))
    vectors, diagonal = orthonormal(dot(previous, cover[...], ((1,), (0,))))
    for i in range(nc):
        vecs[i] = vectors[:, i * width : (i + 1) * width]
    right_ref[...] = vecs[col]
    strength_ref[...] = diagonal[:, : strength_ref.shape[1]] / (rows_dev * na * nb)
    for k in range(LEFT_CHUNKS):
        for h, m in enumerate(moved[k]):
            m.wait()
            q = lax.rem(hi + nh - (h + 1), nh) * CORES + core
            place = pl.ds(aligned(q * quarter + k * rows, 128), rows)
            sent.append(remote(left_ref.at[:, place], left_ref.at[:, place], at_core(peer)))
    for s in sent:
        s.wait()
    assert used[0] <= n_copies, used


def solution(mesh):
    na, nb, nc = mesh.shape["rowa"], mesh.shape["rowb"], mesh.shape["col"]
    nh = nc // CORES

    def on_device(table, start):
        rows_dev, width = table.shape
        block = start.shape[0]
        quarter, half = rows_dev // nc, CORES * width
        f32 = jnp.float32
        n_copies = 256
        vmem = pltpu.VMEM
        quad = half // CORES
        right, left, strength = pl.pallas_call(
            functools.partial(kernel, na, nb, nc, n_copies),
            out_shape=(
                jax.ShapeDtypeStruct((block, width), f32),
                jax.ShapeDtypeStruct((block, rows_dev), f32),
                jax.ShapeDtypeStruct((1, block), f32),
            ),
            in_specs=[pl.BlockSpec(memory_space=pl.ANY), pl.BlockSpec(memory_space=pltpu.VMEM)],
            out_specs=tuple([pl.BlockSpec(memory_space=pltpu.VMEM)] * 3),
            scratch_shapes=[
                vmem((nc, quarter, width), f32),
                vmem((nh - 1, CORES, quarter, width), f32),
                vmem((nc, block, width), f32),
                vmem((half, half), f32),
                vmem((half, half), f32),
                vmem((nh, half, half), f32),
                vmem((half, half), f32),
                vmem((nc * width, nc * width), f32),
                vmem((CORES - 1, quad, half), f32),
                vmem((na - 1, quad // na, half), f32),
                vmem((nb, quad // na, half), f32),
                vmem((CORES - 1, quad, half), f32),
                vmem((nh - 1, quad // nh, half), f32),
                vmem((na - 1, quad // nh // na, half), f32),
                vmem((nb, quad // nh // na, half), f32),
                pltpu.SemaphoreType.DMA((n_copies,)),
                pltpu.SemaphoreType.DMA((n_copies,)),
                pltpu.SemaphoreType.DMA((nh,)),
            ],
            compiler_params=pltpu.CompilerParams(
                collective_id=0, has_side_effects=True, vmem_limit_bytes=48 * 1024 * 1024
            ),
        )(table, start)
        return right, left, strength.reshape(block)

    return jax.shard_map(
        on_device,
        mesh=mesh,
        in_specs=(P(("rowa", "rowb"), "col"), P(None, "col")),
        out_specs=(P(None, "col"), P(None, ("rowa", "rowb")), P()),
        check_vma=False,
    )
```

```python
import functools

import jax
import jax.numpy as jnp
from jax import lax
from jax.experimental import pallas as pl
from jax.experimental.pallas import tpu as pltpu
from jax.sharding import PartitionSpec as P

STEPS = 8
CHUNKS = 8
LEFT_CHUNKS = 4
CORES = 2
MESH = pl.DeviceIdType.MESH
high = lax.Precision.HIGHEST


def dot(a, b, dims):
    return lax.dot_general(a, b, (dims, ((), ())), precision=high, preferred_element_type=jnp.float32)


def orthonormal(products):
    block, cols = products.shape
    tiles = cols // 128
    gram = dot(products, products, ((1,), (1,)))
    column = [jnp.broadcast_to(gram[:, k : k + 1], (block, 128)) for k in range(block)]
    part = [products[:, t * 128 : (t + 1) * 128] for t in range(tiles)]
    row = lax.broadcasted_iota(jnp.int32, (block, 128), 0)
    lane = lax.broadcasted_iota(jnp.int32, (1, 128), 1)
    diagonal = jnp.zeros((1, 128), jnp.float32)
    for j in range(block):
        pivot = column[j][j : j + 1, :]
        inverse = lax.rsqrt(pivot)
        inverse = inverse * (1.5 - 0.5 * (pivot * inverse) * inverse)
        diagonal = jnp.where(lane == j, pivot * inverse, diagonal)
        below = jnp.where(row > j, column[j] * inverse, 0.0)
        for t in range(tiles):
            solved = part[t][j : j + 1, :] * inverse
            part[t] = jnp.where(row == j, solved, part[t] - below * solved)
        for k in range(j + 1, block):
            column[k] = column[k] - below * below[k : k + 1, :]
    return jnp.concatenate(part, axis=1), diagonal


def kernel(na, nb, nc, n_copies, table, start, right_ref, left_ref, strength_ref, *scratch):
    (blocks, extra, vecs, acc_d, acc_c, diag, cross, cover,
     d_core, d_a, d_b, c_core, c_group, c_b, held, coarse, fine, send, recv, local) = scratch
    nh = nc // CORES
    rows_dev, width = table.shape
    quarter = rows_dev // nc
    chunk = quarter // CHUNKS
    half = CORES * width
    a, b, col = lax.axis_index("rowa"), lax.axis_index("rowb"), lax.axis_index("col")
    core, hi = lax.rem(col, CORES), lax.div(col, CORES)
    at_a = lambda i: {"rowa": i}
    at_b = lambda i: {"rowb": i}
    at_col = lambda i: {"col": i}
    at_core = lambda i: {"col": hi * CORES + i}
    at_hi = lambda i: {"col": i * CORES + core}
    at_group = lambda i: {"rowa": lax.rem(i, na), "col": lax.div(i, na) * CORES + core}
    used = [0]

    def aligned(x, n):
        return pl.multiple_of(x, n)

    def remote(src, dst, where):
        i = used[0]
        used[0] += 1
        copy = pltpu.make_async_remote_copy(src_ref=src, dst_ref=dst, send_sem=send.at[i], recv_sem=recv.at[i],
                                            device_id=where, device_id_type=MESH)
        copy.start()
        return copy

    peer = 1 - core
    order = [lax.rem(hi + h, nh) * CORES + lax.rem(core + c, CORES) for h in range(1, nh) for c in range(CORES)]
    loads = []

    def load(src, dst):
        copy = pltpu.make_async_copy(src, dst, local.at[len(loads)])
        copy.start()
        loads.append(copy)

    for q in order + [hi * CORES + peer]:
        rows = pl.ds(aligned(q * quarter, 8), quarter)
        load(table.at[rows], held.at[rows])
    load(start, vecs.at[col])
    load(table.at[pl.ds(aligned(col * quarter, 8), quarter)], blocks.at[col])
    for h in range(1, nh):
        q = lax.rem(hi + h, nh) * CORES + core
        load(table.at[pl.ds(aligned(q * quarter, 8), quarter)], extra.at[h - 1, core])
    copies = loads[len(order) + 2 :]

    barrier = pltpu.get_barrier_semaphore()
    others = ([at_a(lax.rem(a + d, na)) for d in range(1, na)] + [at_b(lax.rem(b + d, nb)) for d in range(1, nb)]
              + [at_col(lax.rem(col + d, nc)) for d in range(1, nc)]
              + [at_group(lax.rem(hi + h, nh) * na + lax.rem(a + d, na)) for h in range(1, nh) for d in range(1, na)])
    for other in others:
        pl.semaphore_signal(barrier, inc=1, device_id=other, device_id_type=MESH)
    pl.semaphore_wait(barrier, len(others))

    for c in loads[: len(order) + 2]:
        c.wait()
    near = []
    for d in range(1, nc):
        near.append(remote(vecs.at[col], vecs.at[col], at_col(lax.rem(col + d, nc))))
    far = []
    for k in range(CHUNKS):
        far.append([])
        for h in range(1, nh):
            for c in range(CORES):
                q = lax.rem(hi + h, nh) * CORES + lax.rem(core + c, CORES)
                far[k].append(remote(held.at[pl.ds(aligned(q * quarter + k * chunk, 8), chunk)],
                                     blocks.at[col, pl.ds(k * chunk, chunk)], at_col(q)))
    q = hi * CORES + peer
    near.append(remote(held.at[pl.ds(aligned(q * quarter, 8), quarter)], blocks.at[col], at_core(peer)))
    for h in range(1, nh):
        q = lax.rem(hi + h, nh) * CORES + peer
        near.append(remote(held.at[pl.ds(aligned(q * quarter, 8), quarter)], extra.at[h - 1, core], at_core(peer)))

    def allreduce(acc, out, stages, slots, over_b, gather):
        off, length = 0, half
        trail = []
        for (n, me, at), slot in zip(stages, slots):
            piece = length // n
            moved = []
            for d in range(1, n):
                to = lax.rem(me + d, n)
                moved.append(remote(acc.at[pl.ds(aligned(off + to * piece, 8), piece)], slot.at[d - 1], at(to)))
            yield
            for m in moved:
                m.wait()
            trail.append((off, length))
            off, length = off + me * piece, piece
            mine = pl.ds(aligned(off, 8), length)
            total = acc[mine]
            for d in range(1, n):
                total = total + slot[d - 1]
            acc[mine] = total
        mine = pl.ds(aligned(off, 8), length)
        over_b[b] = acc[mine]
        moved = [remote(over_b.at[b], over_b.at[b], at_b(lax.rem(b + d, nb))) for d in range(1, nb)]
        yield
        for m in moved:
            m.wait()
        total = over_b[0]
        for i in range(1, nb):
            total = total + over_b[i]
        out[mine] = total
        for (n, me, at), (above, longer) in list(zip(stages, trail))[::-1][:gather]:
            mine = pl.ds(aligned(off, 8), length)
            moved = [remote(out.at[mine], out.at[mine], at(lax.rem(me + d, n))) for d in range(1, n)]
            yield
            for m in moved:
                m.wait()
            off, length = above, longer

    def diagonal_parts():
        acc_d[...] = jnp.zeros_like(acc_d)
        for c in copies:
            c.wait()
        for n in near:
            n.wait()

        @pl.loop(0, CHUNKS)
        def _(k):
            rows = pl.ds(aligned(k * chunk, 8), chunk)
            own = jnp.concatenate([blocks[hi * CORES + i, rows] for i in range(CORES)], axis=1)
            total = acc_d[...] + dot(own, own, ((0,), (0,)))
            for h in range(1, nh):
                own = jnp.concatenate([extra[h - 1, i, rows] for i in range(CORES)], axis=1)
                total = total + dot(own, own, ((0,), (0,)))
            acc_d[...] = total

        mine = diag.at[hi]
        yield from allreduce(acc_d, mine, [(CORES, core, at_core), (na, a, at_a)], [d_core, d_a], d_b, 1)
        rows = pl.ds(aligned(core * (half // CORES), 8), half // CORES)
        moved = [remote(mine.at[rows], mine.at[rows], at_hi(lax.rem(hi + h, nh))) for h in range(1, nh)]
        yield
        for m in moved:
            m.wait()
        moved = [remote(diag.at[:, rows], diag.at[:, rows], at_core(peer))]
        yield
        for m in moved:
            m.wait()

    def cross_chunk(k):
        for m in far[k]:
            m.wait()
        rows = pl.ds(k * chunk, chunk)
        whole = jnp.concatenate([blocks[i, rows] for i in range(nc)], axis=1)
        turned = whole.T
        large = turned.astype(jnp.bfloat16)
        coarse[:, rows] = large
        fine[:, rows] = (turned - large.astype(jnp.float32)).astype(jnp.bfloat16)
        new = dot(turned[:half], whole[:, half:], ((1,), (0,)))
        acc_c[...] = new if k == 0 else acc_c[...] + new

    beside = diagonal_parts()
    next(beside)
    for k in range(CHUNKS):
        cross_chunk(k)
        if k < CHUNKS - 1 and k < 4:
            next(beside)
    stages = [(CORES, core, at_core), (nh * na, hi * na + a, at_group)]
    for i, _ in enumerate(allreduce(acc_c, cross, stages, [c_core, c_group], c_b, 2)):
        if i == 3:
            next(beside)
    for _ in beside:
        pass
    for h in range(nh):
        cover[h * half : (h + 1) * half, h * half : (h + 1) * half] = diag[h]
    cover[:half, half:] = cross[...]
    cover[half:, :half] = cross[...].T

    vectors = jnp.concatenate([vecs[i] for i in range(nc)], axis=1)

    def step(_, vectors):
        return orthonormal(dot(vectors, cover[...], ((1,), (0,))))[0]

    previous = lax.fori_loop(0, STEPS - 1, step, vectors)
    moved, sent = [], []
    rows = quarter // LEFT_CHUNKS
    large = previous.astype(jnp.bfloat16)
    small = (previous - large.astype(jnp.float32)).astype(jnp.bfloat16)
    block = previous.shape[0]
    both = jnp.concatenate([large, small], axis=0)
    for k in range(LEFT_CHUNKS):
        piece = pl.ds(k * rows, rows)
        main = jnp.dot(both, coarse[:, piece], preferred_element_type=jnp.float32)
        rest = jnp.dot(large, fine[:, piece], preferred_element_type=jnp.float32)
        place = pl.ds(aligned(col * quarter + k * rows, 128), rows)
        left_ref[:, place] = main[:block] + (main[block:] + rest)
        moved.append([remote(left_ref.at[:, place], left_ref.at[:, place], at_hi(lax.rem(hi + h, nh))) for h in range(1, nh)])
        sent.append(remote(left_ref.at[:, place], left_ref.at[:, place], at_core(peer)))
    vectors, diagonal = orthonormal(dot(previous, cover[...], ((1,), (0,))))
    for i in range(nc):
        vecs[i] = vectors[:, i * width : (i + 1) * width]
    right_ref[...] = vecs[col]
    strength_ref[...] = diagonal[:, : strength_ref.shape[1]] / (rows_dev * na * nb)
    for k in range(LEFT_CHUNKS):
        for h, m in enumerate(moved[k]):
            m.wait()
            q = lax.rem(hi + nh - (h + 1), nh) * CORES + core
            place = pl.ds(aligned(q * quarter + k * rows, 128), rows)
            sent.append(remote(left_ref.at[:, place], left_ref.at[:, place], at_core(peer)))
    for s in sent:
        s.wait()
    assert used[0] <= n_copies, used


def hand_out(*refs):
    sems = refs[-1]
    copies = [pltpu.make_async_copy(refs[i], refs[3 + i], sems.at[i]) for i in range(3)]
    for c in copies:
        c.start()
    for c in copies:
        c.wait()


def solution(mesh):
    na, nb, nc = mesh.shape["rowa"], mesh.shape["rowb"], mesh.shape["col"]
    nh = nc // CORES

    def on_device(table, start):
        rows_dev, width = table.shape
        block = start.shape[0]
        quarter, half = rows_dev // nc, CORES * width
        f32 = jnp.float32
        n_copies = 256
        vmem = pltpu.VMEM
        quad = half // CORES
        right, left, strength = pl.pallas_call(
            functools.partial(kernel, na, nb, nc, n_copies),
            out_shape=(
                jax.ShapeDtypeStruct((block, width), f32),
                jax.ShapeDtypeStruct((block, rows_dev), f32),
                jax.ShapeDtypeStruct((1, block), f32),
            ),
            in_specs=[pl.BlockSpec(memory_space=pl.ANY), pl.BlockSpec(memory_space=pl.ANY)],
            out_specs=tuple([pl.BlockSpec(memory_space=pltpu.VMEM)] * 3),
            scratch_shapes=[
                vmem((nc, quarter, width), f32),
                vmem((nh - 1, CORES, quarter, width), f32),
                vmem((nc, block, width), f32),
                vmem((half, half), f32),
                vmem((half, half), f32),
                vmem((nh, half, half), f32),
                vmem((half, half), f32),
                vmem((nc * width, nc * width), f32),
                vmem((CORES - 1, quad, half), f32),
                vmem((na - 1, quad // na, half), f32),
                vmem((nb, quad // na, half), f32),
                vmem((CORES - 1, quad, half), f32),
                vmem((nh * na - 1, quad // nh // na, half), f32),
                vmem((nb, quad // nh // na, half), f32),
                vmem((rows_dev, width), f32),
                vmem((nc * width, quarter), jnp.bfloat16),
                vmem((nc * width, quarter), jnp.bfloat16),
                pltpu.SemaphoreType.DMA((n_copies,)),
                pltpu.SemaphoreType.DMA((n_copies,)),
                pltpu.SemaphoreType.DMA((nc + nh + 1,)),
            ],
            compiler_params=pltpu.CompilerParams(
                collective_id=0, has_side_effects=True, vmem_limit_bytes=60 * 1024 * 1024
            ),
        )(table, start)
        right, left, strength = pl.pallas_call(
            hand_out,
            out_shape=tuple(jax.ShapeDtypeStruct(x.shape, f32) for x in (right, left, strength)),
            in_specs=[pl.BlockSpec(memory_space=pltpu.VMEM)] * 3,
            out_specs=tuple([pl.BlockSpec(memory_space=pl.ANY)] * 3),
            scratch_shapes=[pltpu.SemaphoreType.DMA((3,))],
        )(right, left, strength)
        return right, left, strength.reshape(block)

    return jax.shard_map(
        on_device,
        mesh=mesh,
        in_specs=(P(("rowa", "rowb"), "col"), P(None, "col")),
        out_specs=(P(None, "col"), P(None, ("rowa", "rowb")), P()),
        check_vma=False,
    )
```

```python
import functools

import jax
import jax.numpy as jnp
from jax import lax
from jax.experimental import pallas as pl
from jax.experimental.pallas import tpu as pltpu
from jax.sharding import PartitionSpec as P

STEPS = 8
CHUNKS = 16
LEFT_CHUNKS = 4
CORES = 2
MESH = pl.DeviceIdType.MESH
high = lax.Precision.HIGHEST


def dot(a, b, dims):
    return lax.dot_general(a, b, (dims, ((), ())), precision=high, preferred_element_type=jnp.float32)


def orthonormal(products):
    block, cols = products.shape
    tiles = cols // 128
    gram = dot(products, products, ((1,), (1,)))
    column = [jnp.broadcast_to(gram[:, k : k + 1], (block, 128)) for k in range(block)]
    part = [products[:, t * 128 : (t + 1) * 128] for t in range(tiles)]
    row = lax.broadcasted_iota(jnp.int32, (block, 128), 0)
    lane = lax.broadcasted_iota(jnp.int32, (1, 128), 1)
    diagonal = jnp.zeros((1, 128), jnp.float32)
    for j in range(block):
        pivot = column[j][j : j + 1, :]
        inverse = lax.rsqrt(pivot)
        inverse = inverse * (1.5 - 0.5 * (pivot * inverse) * inverse)
        diagonal = jnp.where(lane == j, pivot * inverse, diagonal)
        below = jnp.where(row > j, column[j] * inverse, 0.0)
        for t in range(tiles):
            solved = part[t][j : j + 1, :] * inverse
            part[t] = jnp.where(row == j, solved, part[t] - below * solved)
        for k in range(j + 1, block):
            column[k] = column[k] - below * below[k : k + 1, :]
    return jnp.concatenate(part, axis=1), diagonal


def kernel(na, nb, nc, n_copies, table, start, right_ref, left_ref, strength_ref, *scratch):
    (blocks, extra, vecs, acc_d, acc_c, diag, cross, cover,
     d_core, d_a, d_b, c_core, c_group, c_b, held, coarse, fine, send, recv, local) = scratch
    nh = nc // CORES
    rows_dev, width = table.shape
    quarter = rows_dev // nc
    chunk = quarter // CHUNKS
    half = CORES * width
    a, b, col = lax.axis_index("rowa"), lax.axis_index("rowb"), lax.axis_index("col")
    core, hi = lax.rem(col, CORES), lax.div(col, CORES)
    at_a = lambda i: {"rowa": i}
    at_b = lambda i: {"rowb": i}
    at_col = lambda i: {"col": i}
    at_core = lambda i: {"col": hi * CORES + i}
    at_hi = lambda i: {"col": i * CORES + core}
    at_group = lambda i: {"rowa": lax.rem(i, na), "col": lax.div(i, na) * CORES + core}
    used = [0]

    def aligned(x, n):
        return pl.multiple_of(x, n)

    def remote(src, dst, where):
        i = used[0]
        used[0] += 1
        copy = pltpu.make_async_remote_copy(src_ref=src, dst_ref=dst, send_sem=send.at[i], recv_sem=recv.at[i],
                                            device_id=where, device_id_type=MESH)
        copy.start()
        return copy

    peer = 1 - core
    order = [lax.rem(hi + h, nh) * CORES + lax.rem(core + c, CORES) for h in range(1, nh) for c in range(CORES)]
    loads = []

    def load(src, dst):
        copy = pltpu.make_async_copy(src, dst, local.at[len(loads)])
        copy.start()
        loads.append(copy)

    for q in order + [hi * CORES + peer]:
        rows = pl.ds(aligned(q * quarter, 8), quarter)
        load(table.at[rows], held.at[rows])
    load(start, vecs.at[col])
    load(table.at[pl.ds(aligned(col * quarter, 8), quarter)], blocks.at[col])
    for h in range(1, nh):
        q = lax.rem(hi + h, nh) * CORES + core
        load(table.at[pl.ds(aligned(q * quarter, 8), quarter)], extra.at[h - 1, core])
    copies = loads[len(order) + 2 :]

    barrier = pltpu.get_barrier_semaphore()
    others = ([at_a(lax.rem(a + d, na)) for d in range(1, na)] + [at_b(lax.rem(b + d, nb)) for d in range(1, nb)]
              + [at_col(lax.rem(col + d, nc)) for d in range(1, nc)]
              + [at_group(lax.rem(hi + h, nh) * na + lax.rem(a + d, na)) for h in range(1, nh) for d in range(1, na)])
    for other in others:
        pl.semaphore_signal(barrier, inc=1, device_id=other, device_id_type=MESH)
    pl.semaphore_wait(barrier, len(others))

    for c in loads[: len(order) + 2]:
        c.wait()
    near = []
    for d in range(1, nc):
        near.append(remote(vecs.at[col], vecs.at[col], at_col(lax.rem(col + d, nc))))
    far = []
    for k in range(CHUNKS):
        far.append([])
        for h in range(1, nh):
            for c in range(CORES):
                q = lax.rem(hi + h, nh) * CORES + lax.rem(core + c, CORES)
                far[k].append(remote(held.at[pl.ds(aligned(q * quarter + k * chunk, 8), chunk)],
                                     blocks.at[col, pl.ds(k * chunk, chunk)], at_col(q)))
    q = hi * CORES + peer
    near.append(remote(held.at[pl.ds(aligned(q * quarter, 8), quarter)], blocks.at[col], at_core(peer)))
    for h in range(1, nh):
        q = lax.rem(hi + h, nh) * CORES + peer
        near.append(remote(held.at[pl.ds(aligned(q * quarter, 8), quarter)], extra.at[h - 1, core], at_core(peer)))

    def allreduce(acc, out, stages, slots, over_b, gather):
        off, length = 0, half
        trail = []
        for (n, me, at), slot in zip(stages, slots):
            piece = length // n
            moved = []
            for d in range(1, n):
                to = lax.rem(me + d, n)
                moved.append(remote(acc.at[pl.ds(aligned(off + to * piece, 8), piece)], slot.at[d - 1], at(to)))
            yield
            for m in moved:
                m.wait()
            trail.append((off, length))
            off, length = off + me * piece, piece
            mine = pl.ds(aligned(off, 8), length)
            total = acc[mine]
            for d in range(1, n):
                total = total + slot[d - 1]
            acc[mine] = total
        mine = pl.ds(aligned(off, 8), length)
        over_b[b] = acc[mine]
        moved = [remote(over_b.at[b], over_b.at[b], at_b(lax.rem(b + d, nb))) for d in range(1, nb)]
        yield
        for m in moved:
            m.wait()
        total = over_b[0]
        for i in range(1, nb):
            total = total + over_b[i]
        out[mine] = total
        for (n, me, at), (above, longer) in list(zip(stages, trail))[::-1][:gather]:
            mine = pl.ds(aligned(off, 8), length)
            moved = [remote(out.at[mine], out.at[mine], at(lax.rem(me + d, n))) for d in range(1, n)]
            yield
            for m in moved:
                m.wait()
            off, length = above, longer

    def diagonal_parts():
        acc_d[...] = jnp.zeros_like(acc_d)
        for c in copies:
            c.wait()
        for n in near:
            n.wait()

        @pl.loop(0, CHUNKS)
        def _(k):
            rows = pl.ds(aligned(k * chunk, 8), chunk)
            own = jnp.concatenate([blocks[hi * CORES + i, rows] for i in range(CORES)], axis=1)
            total = acc_d[...] + dot(own, own, ((0,), (0,)))
            for h in range(1, nh):
                own = jnp.concatenate([extra[h - 1, i, rows] for i in range(CORES)], axis=1)
                total = total + dot(own, own, ((0,), (0,)))
            acc_d[...] = total

        mine = diag.at[hi]
        yield from allreduce(acc_d, mine, [(CORES, core, at_core), (na, a, at_a)], [d_core, d_a], d_b, 1)
        rows = pl.ds(aligned(core * (half // CORES), 8), half // CORES)
        moved = [remote(mine.at[rows], mine.at[rows], at_hi(lax.rem(hi + h, nh))) for h in range(1, nh)]
        yield
        for m in moved:
            m.wait()
        moved = [remote(diag.at[:, rows], diag.at[:, rows], at_core(peer))]
        yield
        for m in moved:
            m.wait()

    def cross_chunk(k):
        for m in far[k]:
            m.wait()
        rows = pl.ds(k * chunk, chunk)
        whole = jnp.concatenate([blocks[i, rows] for i in range(nc)], axis=1)
        turned = whole.T
        large = turned.astype(jnp.bfloat16)
        coarse[:, rows] = large
        fine[:, rows] = (turned - large.astype(jnp.float32)).astype(jnp.bfloat16)
        new = dot(turned[:half], whole[:, half:], ((1,), (0,)))
        acc_c[...] = new if k == 0 else acc_c[...] + new

    beside = diagonal_parts()
    next(beside)
    for k in range(CHUNKS):
        cross_chunk(k)
        if k < CHUNKS - 1 and k < 4:
            next(beside)
    stages = [(CORES, core, at_core), (nh * na, hi * na + a, at_group)]
    for i, _ in enumerate(allreduce(acc_c, cross, stages, [c_core, c_group], c_b, 2)):
        if i == 3:
            next(beside)
    for _ in beside:
        pass
    for h in range(nh):
        cover[h * half : (h + 1) * half, h * half : (h + 1) * half] = diag[h]
    cover[:half, half:] = cross[...]
    cover[half:, :half] = cross[...].T

    vectors = jnp.concatenate([vecs[i] for i in range(nc)], axis=1)

    def step(_, vectors):
        return orthonormal(dot(vectors, cover[...], ((1,), (0,))))[0]

    previous = lax.fori_loop(0, STEPS - 1, step, vectors)
    moved, sent = [], []
    rows = quarter // LEFT_CHUNKS
    large = previous.astype(jnp.bfloat16)
    small = (previous - large.astype(jnp.float32)).astype(jnp.bfloat16)
    block = previous.shape[0]
    both = jnp.concatenate([large, small], axis=0)
    for k in range(LEFT_CHUNKS):
        piece = pl.ds(k * rows, rows)
        main = jnp.dot(both, coarse[:, piece], preferred_element_type=jnp.float32)
        rest = jnp.dot(large, fine[:, piece], preferred_element_type=jnp.float32)
        place = pl.ds(aligned(col * quarter + k * rows, 128), rows)
        left_ref[:, place] = main[:block] + (main[block:] + rest)
        moved.append([remote(left_ref.at[:, place], left_ref.at[:, place], at_hi(lax.rem(hi + h, nh))) for h in range(1, nh)])
        sent.append(remote(left_ref.at[:, place], left_ref.at[:, place], at_core(peer)))
    vectors, diagonal = orthonormal(dot(previous, cover[...], ((1,), (0,))))
    for i in range(nc):
        vecs[i] = vectors[:, i * width : (i + 1) * width]
    right_ref[...] = vecs[col]
    strength_ref[...] = diagonal[:, : strength_ref.shape[1]] / (rows_dev * na * nb)
    for k in range(LEFT_CHUNKS):
        for h, m in enumerate(moved[k]):
            m.wait()
            q = lax.rem(hi + nh - (h + 1), nh) * CORES + core
            place = pl.ds(aligned(q * quarter + k * rows, 128), rows)
            sent.append(remote(left_ref.at[:, place], left_ref.at[:, place], at_core(peer)))
    for s in sent:
        s.wait()
    assert used[0] <= n_copies, used


def hand_out(*refs):
    sems = refs[-1]
    copies = [pltpu.make_async_copy(refs[i], refs[3 + i], sems.at[i]) for i in range(3)]
    for c in copies:
        c.start()
    for c in copies:
        c.wait()


def solution(mesh):
    na, nb, nc = mesh.shape["rowa"], mesh.shape["rowb"], mesh.shape["col"]
    nh = nc // CORES

    def on_device(table, start):
        rows_dev, width = table.shape
        block = start.shape[0]
        quarter, half = rows_dev // nc, CORES * width
        f32 = jnp.float32
        n_copies = 256
        vmem = pltpu.VMEM
        quad = half // CORES
        right, left, strength = pl.pallas_call(
            functools.partial(kernel, na, nb, nc, n_copies),
            out_shape=(
                jax.ShapeDtypeStruct((block, width), f32),
                jax.ShapeDtypeStruct((block, rows_dev), f32),
                jax.ShapeDtypeStruct((1, block), f32),
            ),
            in_specs=[pl.BlockSpec(memory_space=pl.ANY), pl.BlockSpec(memory_space=pl.ANY)],
            out_specs=tuple([pl.BlockSpec(memory_space=pltpu.VMEM)] * 3),
            scratch_shapes=[
                vmem((nc, quarter, width), f32),
                vmem((nh - 1, CORES, quarter, width), f32),
                vmem((nc, block, width), f32),
                vmem((half, half), f32),
                vmem((half, half), f32),
                vmem((nh, half, half), f32),
                vmem((half, half), f32),
                vmem((nc * width, nc * width), f32),
                vmem((CORES - 1, quad, half), f32),
                vmem((na - 1, quad // na, half), f32),
                vmem((nb, quad // na, half), f32),
                vmem((CORES - 1, quad, half), f32),
                vmem((nh * na - 1, quad // nh // na, half), f32),
                vmem((nb, quad // nh // na, half), f32),
                vmem((rows_dev, width), f32),
                vmem((nc * width, quarter), jnp.bfloat16),
                vmem((nc * width, quarter), jnp.bfloat16),
                pltpu.SemaphoreType.DMA((n_copies,)),
                pltpu.SemaphoreType.DMA((n_copies,)),
                pltpu.SemaphoreType.DMA((nc + nh + 1,)),
            ],
            compiler_params=pltpu.CompilerParams(
                collective_id=0, has_side_effects=True, vmem_limit_bytes=60 * 1024 * 1024
            ),
        )(table, start)
        right, left, strength = pl.pallas_call(
            hand_out,
            out_shape=tuple(jax.ShapeDtypeStruct(x.shape, f32) for x in (right, left, strength)),
            in_specs=[pl.BlockSpec(memory_space=pltpu.VMEM)] * 3,
            out_specs=tuple([pl.BlockSpec(memory_space=pl.ANY)] * 3),
            scratch_shapes=[pltpu.SemaphoreType.DMA((3,))],
        )(right, left, strength)
        return right, left, strength.reshape(block)

    return jax.shard_map(
        on_device,
        mesh=mesh,
        in_specs=(P(("rowa", "rowb"), "col"), P(None, "col")),
        out_specs=(P(None, "col"), P(None, ("rowa", "rowb")), P()),
        check_vma=False,
    )
```
